32 devices in a mesh: rows: 16 (over z, x, core), inner: 2 (over y).
Axes of the slice: x: 2, y: 2, z: 4, core: 2. Of those that a mesh axis runs over, the one named last changes fastest.
Arguments:
- blocks: bfloat16 [16, 16, 256, 256], P('rows'), may hold values from -0.375 to 0.375
- columns: int32 [16, 16], replicated, may hold values from -1 to 15, as said below
Outputs:
- purified: float32 [16, 16, 256, 256], P('rows', None, 'inner')
The draws below stay inside these ranges and needn't reach their ends.
Inputs may be any that keep to these rules, and one draw needn't show every extreme that they name: Each entry of row i that is not -1 is (i + d) mod 16 for an offset d with -16 <= 2 * d < 16; the entries of a row are distinct and stand before its -1 entries; every row lists its diagonal block; some row lists 16 columns.
All inputs are finite; a program needn't handle non-finite values.
Results may differ from the reference program's by a relative error of at most 0.0055.
Values may be sent and summed in bfloat16 or wider, within the bound.
A program may use at most 128 MiB of HBM per device.

```python
import jax
import jax.numpy as jnp
from jax import lax

BS = 256
BAND = 16
NB = 16
N_INNER = 2


def draw_columns(key, part):
    half_band = BAND // 2
    first_key, second_key, third_key = jax.random.split(jax.random.fold_in(key, 11), 3)
    density = jax.random.randint(first_key, (NB, 1), 24, 96)
    rolls = jax.random.randint(second_key, (NB, BAND), 0, 64)
    slot_ids = jnp.arange(BAND, dtype=jnp.int32)
    distance = 3 * jnp.abs(slot_ids - half_band)
    live_slots = rolls < density - distance[None, :]
    full_row = jax.random.randint(third_key, (), 0, NB)
    row_ids = jnp.arange(NB, dtype=jnp.int32)
    live_slots = live_slots | (slot_ids[None, :] == half_band) | (row_ids[:, None] == full_row)
    sort_keys = jnp.where(live_slots, slot_ids[None, :], slot_ids[None, :] + BAND)
    order = jnp.argsort(sort_keys, axis=1, stable=True).astype(jnp.int32)
    live_sorted = jnp.take_along_axis(live_slots, order, axis=1)
    block_cols = (row_ids[:, None] + order - half_band) % NB
    return jnp.where(live_sorted, block_cols, -1).astype(jnp.int32)


def block_levels(key, dims, shards, least, largest):
    factor_of, own = 1.0, jax.random.fold_in(key, 6)
    for axis_at, shards_of in shards:
        heights = jnp.exp(jax.random.uniform(jax.random.fold_in(own, axis_at), (shards_of,), jnp.float32, least / len(shards), largest / len(shards)))
        factor_of = factor_of * jnp.repeat(heights, dims[axis_at] // shards_of).reshape([-1 if axis == axis_at else 1 for axis in range(len(dims))])
    return factor_of


def gaussian(stream_key, shape, width, reach, cuts=(), held_as=jnp.bfloat16):
    entries = width * jax.random.normal(stream_key, shape, jnp.float32)
    if cuts:
        entries = entries * block_levels(stream_key, shape, cuts, -0.22, 0.18)
    return jnp.clip(entries, -reach, reach).astype(held_as)


def setup_inputs(seed: int = 0) -> dict:
    arg_keys = jax.random.split(jax.random.key(seed), 3)
    blocks = gaussian(arg_keys[0], (NB, BAND, BS, BS), BS ** -0.5, 0.375, ((0, 16),))
    columns = draw_columns(jax.random.fold_in(arg_keys[2], 71), 0)
    return dict(blocks=blocks, columns=columns)


def live_table(columns):
    nrows, band_width = columns.shape
    half_band = band_width // 2
    row_ids = jnp.arange(nrows, dtype=jnp.int32)
    target = (row_ids[:, None] + jnp.arange(band_width, dtype=jnp.int32)[None, :] - half_band) % nrows
    return jnp.any(columns[:, None, :] == target[:, :, None], axis=2)


def slot_shift(piece, delta):
    band_width = piece.shape[1]
    if delta >= 0:
        return jnp.concatenate([piece[:, delta:], jnp.zeros_like(piece[:, :delta])], axis=1)
    return jnp.concatenate([jnp.zeros_like(piece[:, :(-delta)]), piece[:, :band_width + delta]], axis=1)


def band_product(left_all, right_all):
    nrows, band_width, block_size, _ = left_all.shape
    half_band = band_width // 2
    slab_width = block_size // N_INNER

    def one_row(row_index):
        row_ids = (row_index + jnp.arange(band_width, dtype=jnp.int32) - half_band) % nrows
        right_rows = right_all[row_ids]
        left_rows = left_all[row_index]
        totals = jnp.zeros((N_INNER, band_width, block_size, block_size), jnp.float32)
        for offset in range(band_width):
            shifted = slot_shift(right_rows[offset][None], half_band - offset)[0]
            left_slab = left_rows[offset].astype(jnp.float32).reshape(block_size, N_INNER, slab_width)
            right_slab = shifted.astype(jnp.float32).reshape(band_width, N_INNER, slab_width, block_size)
            totals = totals + jnp.einsum("mcq,scqn->csmn", left_slab, right_slab)
        rounded = lax.optimization_barrier(totals.astype(jnp.bfloat16))
        return jnp.sum(rounded.astype(jnp.float32), axis=0)

    return lax.map(one_row, jnp.arange(nrows, dtype=jnp.int32))


def reference(blocks, columns):
    live_slots = live_table(columns)[:, :, None, None]
    masked = jnp.where(live_slots, blocks, jnp.zeros_like(blocks))
    square = jnp.where(live_slots, band_product(masked, masked), jnp.float32(0.0)).astype(jnp.bfloat16)
    cubed = jnp.where(live_slots, band_product(masked, square), jnp.float32(0.0))
    return 3.0 * square.astype(jnp.float32) - 2.0 * cubed
```

```python
import functools

import jax
import jax.numpy as jnp
from jax import lax
from jax.experimental import pallas as pl
from jax.experimental.pallas import tpu as pltpu
from jax.sharding import PartitionSpec as P

MESH = pl.DeviceIdType.MESH

WINDOW = 3
EXTRA = ((0, 0),)
GROUP = ((0, 0), (1, 0), (0, 1), (1, 1))
ORDER = (
    ("x", 1, 1, 0, 0), ("x", 1, 1, 0, 1), ("l", 1, 0, 0, 0, 0), ("l", 1, 0, 0, 0, 1), ("p", 4, 0),
("p", 4, 1), ("x", 0, 0, 0, 0), ("x", 0, 0, 0, 1), ("l", 2, 0, 1, 0, 0), ("l", 2, 0, 1, 0, 1),
("x", 1, 0, 0, 0), ("x", 1, 0, 0, 1), ("l", 1, 1, 0, 0, 0), ("l", 1, 1, 0, 0, 1), ("p", 5, 0), ("p", 5, 1),
("l", 3, 0, 0, 0, 0), ("l", 3, 0, 0, 0, 1), ("l", 2, 0, 0, 0, 0), ("l", 2, 0, 0, 0, 1),
("l", 1, 0, 1, 0, 0), ("l", 1, 0, 1, 0, 1), ("x", 0, 0, 1, 0), ("x", 0, 0, 1, 1), ("l", 1, 1, 1, 0, 0),
("l", 1, 1, 1, 0, 1), ("p", 7, 0), ("p", 7, 1), ("l", 3, 0, 1, 0, 0), ("l", 3, 0, 1, 0, 1), ("p", 6, 0),
("p", 6, 1), ("l", 2, 1, 1, 0, 0), ("l", 2, 1, 1, 0, 1), ("p", 8, 0), ("p", 8, 1), ("p", 9, 0), ("p", 9, 1),
("p", 10, 0), ("p", 10, 1), ("p", 11, 0), ("p", 11, 1), ("p", 12, 0), ("p", 12, 1), ("p", 13, 0),
("p", 13, 1), ("p", 14, 0), ("p", 14, 1), ("p", 15, 0), ("p", 15, 1), ("s", 0), ("l", 3, 1, 0, 0, 0),
("l", 3, 1, 0, 0, 1), ("l", 1, 0, 0, 1, 0), ("l", 1, 0, 0, 1, 1), ("l", 1, 1, 0, 1, 0),
("l", 1, 1, 0, 1, 1), ("l", 1, 0, 1, 1, 0), ("l", 1, 0, 1, 1, 1), ("l", 1, 1, 1, 1, 0),
("l", 1, 1, 1, 1, 1), ("s", 1), ("l", 2, 1, 0, 0, 0), ("l", 2, 1, 0, 0, 1), ("q", 4, 0), ("q", 4, 1),
("l", 3, 1, 1, 0, 0), ("l", 3, 1, 1, 0, 1), ("l", 2, 0, 1, 1, 0), ("l", 2, 0, 1, 1, 1),
("l", 2, 0, 0, 1, 0), ("l", 2, 0, 0, 1, 1), ("l", 2, 1, 1, 1, 0), ("l", 2, 1, 1, 1, 1),
("l", 2, 1, 0, 1, 0), ("l", 2, 1, 0, 1, 1), ("s", 2), ("q", 5, 0), ("q", 5, 1), ("l", 3, 0, 0, 1, 0),
("l", 3, 0, 0, 1, 1), ("l", 3, 0, 1, 1, 0), ("l", 3, 0, 1, 1, 1), ("l", 3, 1, 0, 1, 0),
("l", 3, 1, 0, 1, 1), ("l", 3, 1, 1, 1, 0), ("l", 3, 1, 1, 1, 1), ("s", 3), ("c", 0, 1), ("c", 2, 3),
("c", 4, 5), ("c", 8, 9), ("c", 12, 13), ("q", 6, 0), ("q", 6, 1), ("c", 6, 10), ("q", 7, 0), ("q", 7, 1),
("c", 11, 14), ("c", 7), ("c", 15),
)


def grid_kernel(columns, raw, out, left, panels, acc, pure, final, keep_lanes, load_sem,
                left_send, left_recv, panel_send, panel_recv, end_send, end_recv):
    band, block = raw.shape[0], raw.shape[1]
    slab = block // 2
    rank, y = lax.axis_index("rows"), lax.axis_index("inner")
    core, x, low, high = rank % 2, (rank // 2) % 2, (rank // 4) % 2, rank // 8
    other_y = 1 - y

    def flip(bit, by):
        return 1 - bit if by else bit

    def row_at(core_by, x_by, low_by, high_by):
        return 8 * flip(high, high_by) + 4 * flip(low, low_by) + 2 * flip(x, x_by) + flip(core, core_by)

    group_rows = [row_at(0, x_by, 0, high_by) for x_by, high_by in GROUP]
    at_y = {"rows": rank, "inner": other_y}
    at_core = {"rows": row_at(1, 0, 0, 0), "inner": y}
    at_x = {"rows": group_rows[1], "inner": y}
    at_near = {"rows": row_at(0, 0, 1, 0), "inner": y}
    at_far = {"rows": group_rows[2], "inner": y}
    at_xy = {"rows": group_rows[1], "inner": other_y}
    at_far_y = {"rows": group_rows[2], "inner": other_y}
    at_far_x = {"rows": group_rows[3], "inner": y}
    at_far_xy = {"rows": group_rows[3], "inner": other_y}
    everyone = (at_y, at_core, at_x, at_near, at_far, at_xy, at_far_y, at_far_x, at_far_xy)

    barrier = pltpu.get_barrier_semaphore()
    for device in everyone:
        pl.semaphore_signal(barrier, inc=1, device_id=device, device_id_type=MESH)

    loads = []
    for slot in range(band):
        column = (rank + slot + band // 2) % band
        load = pltpu.make_async_copy(raw.at[slot], left.at[0, column], load_sem.at[slot])
        load.start()
        loads.append(load)

    sent = []

    def remote(source, target, send_sem, recv_sem, device):
        return pltpu.make_async_remote_copy(
            src_ref=source, dst_ref=target, send_sem=send_sem, recv_sem=recv_sem, device_id=device, device_id_type=MESH
        )

    def only(wanted, act):
        if wanted is None:
            act()
        else:
            pl.when(wanted)(act)

    def go(copy, wanted=None):
        only(wanted, copy.start)
        sent.append((copy, wanted))

    def column_of(high_by, x_by, y_by, part):
        return 2 * (4 * flip(high, high_by) + 2 * flip(x, x_by) + flip(y, y_by)) + part

    mine = column_of(0, 0, 0, 0)

    def is_read(row, inner_row, first, count):
        s = (first - row + band + band // 2) % band
        a = (inner_row - row + band + band // 2) % band
        return (s + count > band) | ((a - s <= band // 2 - 1 + count) & (s - a <= band // 2 - 1))

    def read_by(which, at, flow, y_by):
        row = group_rows[which]
        if flow == "y":
            return is_read(row, at, column_of(0, 0, 1, 0), 2)
        if y_by:
            return is_read(row, at, column_of(0, 1, 0, 0), 2)
        return is_read(row, at, 2 * (4 * high + 2 * (1 - x)), 4)

    def is_live(row, slot):
        target = (row + slot + band // 2) % band
        found = columns[row, 0] == target
        for at in range(1, columns.shape[1]):
            found = found | (columns[row, at] == target)
        return jnp.where(found, 1, 0)

    def send_left(flow, source, target, device, at, wanted):
        go(remote(left.at[source, at], left.at[target, at], left_send.at[flow, at], left_recv.at[target, at], device), wanted)

    def to_x(source, high_by, x_by, y_by, part):
        at = column_of(high_by, x_by, y_by, part)
        panel = (high_by, x_by, y_by) == (0, 1, 0)
        wanted = None if panel else read_by(source, at, "x", y_by)
        send_left(1 if source == 0 else 2, source, source + 1, at_x, at, wanted)

    def by_x(which, high_by, x_by, y_by):
        return y_by == 0 or (which == 1 and (high_by, 1 - x_by) in EXTRA)

    done = set()

    def take(which, high_by, x_by, y_by, part):
        key = ("left", which, high_by, x_by, y_by, part)
        if key in done:
            return
        done.add(key)
        at = column_of(high_by, x_by, y_by, part)
        ref = left.at[which, at]
        copy = remote(ref, ref, left_send.at[0, at], left_recv.at[which, at], at_y)
        wanted = None
        if y_by:
            wanted = is_read(group_rows[which], at, mine, 2)
        elif which != 2 and (high_by, x_by) != (0, 0):
            wanted = is_read(group_rows[which], at, 2 * (4 * high + 2 * x), 4)
        only(wanted, copy.wait_recv)
        if y_by:
            return
        if (high_by, x_by) == (0, 0):
            own_panel(which, part)
        if which == 2 and fars:
            to_far(*fars.pop(0))
        if which == 2:
            to_x(2, high_by, x_by, 0, part)
        if not (which == 1 and (high_by, 1 - x_by) in EXTRA):
            send_left(2 + which, which, which, at_y, at, read_by(which, at, "y", 0))

    def send_panel(product, source, target, part, device):
        own = product == 0 and source < 4
        ref = left.at[source, mine + part] if own else panels.at[product, source, part]
        go(remote(ref, panels.at[product, target, part], panel_send.at[product, source, target // 8, part],
                  panel_recv.at[product, target, part], device))

    def share(product, which, part):
        send_panel(product, which, 4 + which, part, at_near)
        send_panel(product, which, 8 + which, part, at_core)

    def take_panel(product, source, part):
        key = ("panel", product, source, part)
        if key in done:
            return
        done.add(key)
        ref = panels.at[product, source, part]
        remote(ref, ref, panel_send.at[product, 0, 0, 0], panel_recv.at[product, source, part], at_core).wait_recv()
        if source < 8:
            send_panel(product, source, 8 + source, part, at_core)

    def own_panel(which, part):
        panels[0, which, part] = left[which, mine + part]
        share(0, which, part)

    def apart(a, b):
        return a + b - 2 * a * b

    def source_of(row):
        return (8 * apart(row % 2, core) + 4 * apart((row // 4) % 2, low)
                + 2 * apart(row // 8, high) + apart((row // 2) % 2, x))

    def row_of(source):
        return (8 * apart((source // 2) % 2, high) + 4 * apart((source // 4) % 2, low)
                + 2 * apart(source % 2, x) + apart(source // 8, core))

    def mac(product, which, inner_row, source, part):
        row = group_rows[which]
        valid = is_read(row, inner_row, mine + part, 1)
        term = jnp.dot(left[which, inner_row], panels[product, source, part], preferred_element_type=jnp.float32)
        acc[product, which, part] += jnp.where(valid, term, 0.0)

    def take_row(which):
        for high_by in range(2 if which else 0):
            for x_by in range(2):
                for y_by in range(2):
                    for part in range(2):
                        take(which, high_by, x_by, y_by, part)

    def square_macs(which):
        def body(n, carry):
            for step in range(2):
                inner_row = 2 * n + step
                for part in range(2):
                    mac(0, which, inner_row, source_of(inner_row), part)
            return carry

        lax.fori_loop(0, band // 2, body, 0)

    def cube_macs(*sources):
        for which in range(4):
            take_row(which)
        for source in sources:
            if source < 4:
                assert source in done
                continue
            for part in range(2):
                take_panel(1, source, part)

        def body(n, carry):
            source = sources[0] + (sources[1] - sources[0]) * n if len(sources) > 1 else sources[0]
            for which in range(4):
                for part in range(2):
                    mac(1, which, row_of(source), source, part)
            return carry

        lax.fori_loop(0, len(sources), body, 0)

    def masked(product, which, part):
        keep = keep_lanes[2 * which + part : 2 * which + part + 1] > 0
        return jnp.where(keep, acc[product, which, part], 0.0)

    def square(which):
        for source in range(1, 4):
            for part in range(2):
                take(source, 0, 0, 0, part)
        for source in range(4, 16):
            for part in range(2):
                take_panel(0, source, part)
        take_row(which)
        square_macs(which)
        done.add(which)
        for part in range(2):
            panels[1, which, part] = masked(0, which, part).astype(panels.dtype)
            share(1, which, part)

    def mask_slot(slot, carry):
        column = (rank + slot + band // 2) % band
        keep = jnp.full((1, block), is_live(rank, slot)) > 0
        value = left[0, column]
        left[0, column] = jnp.where(keep, value, jnp.zeros_like(value))
        return carry

    for load in loads:
        load.wait()
    lax.fori_loop(0, band, mask_slot, 0)
    pl.semaphore_wait(barrier, len(everyone))

    def to_far(high_by, x_by, part):
        at = column_of(high_by, x_by, 0, part)
        send_left(0, 0, 2, at_far, at, None)

    fars = [(high_by, x_by, part) for high_by, x_by in ((1, 1), (1, 0), (0, 1), (0, 0)) for part in range(2)]
    for _ in range(WINDOW):
        to_far(*fars.pop(0))
    for part in range(2):
        to_x(0, 0, 1, 0, part)
        own_panel(0, part)
    for which in range(4):
        for part in range(2):
            row = group_rows[which]
            live = is_live(row, (mine + part - row + band + band // 2) % band)
            at = 2 * which + part
            keep_lanes[at : at + 1] = jnp.full((1, block), live)
    acc[...] = jnp.zeros_like(acc)

    acts = {"x": lambda a, b, w, t: to_x(0, a, b, w, t), "l": take, "p": lambda s, t: take_panel(0, s, t),
            "q": lambda s, t: take_panel(1, s, t), "s": square, "c": cube_macs}
    for name, *numbers in ORDER:
        acts[name](*numbers)

    here = pl.ds(pl.multiple_of(y * slab, slab), slab)
    there = pl.ds(pl.multiple_of(other_y * slab, slab), slab)

    def end(which, half, device):
        at = 2 * which + half
        rows = there if half else here
        go(remote(pure.at[which, :, rows], final.at[pl.ds(mine, 2)], end_send.at[at], end_recv.at[at], device))

    ends = {0: ((1, at_y),), 1: ((1, at_xy), (0, at_x)), 2: ((1, at_far_y), (0, at_far)), 3: ((1, at_far_xy), (0, at_far_x))}
    for which in (3, 2, 1, 0):
        for part in range(2):
            total = 3.0 * panels[1, which, part].astype(jnp.float32) - 2.0 * masked(1, which, part)
            pure[which, part] = total.astype(pure.dtype)
        for half, device in ends[which]:
            end(which, half, device)

    def place(value, column):
        out[(column - rank + band + band // 2) % band] = value

    for part in range(2):
        place(pure[0, part, here], mine + part)
    for which in range(4):
        for half, _ in ends[which]:
            x_by, high_by = GROUP[which]
            at = column_of(high_by, x_by, half, 0)
            ref = final.at[pl.ds(at, 2)]
            remote(ref, ref, end_send.at[0], end_recv.at[2 * which + half], at_y).wait_recv()
            for part in range(2):
                place(final[at + part], at + part)
    for copy, wanted in sent:
        only(wanted, copy.wait_send)


def on_grid(blocks, columns):
    _, band, block, _ = blocks.shape
    vmem = pl.BlockSpec(memory_space=pltpu.VMEM)
    dma = pltpu.SemaphoreType.DMA
    result = pl.pallas_call(
        grid_kernel,
        out_shape=jax.ShapeDtypeStruct((band, block // 2, block), blocks.dtype),
        in_specs=[pl.BlockSpec(memory_space=pltpu.SMEM), pl.BlockSpec(memory_space=pl.ANY)],
        out_specs=vmem,
        scratch_shapes=[
            pltpu.VMEM((4, band, block, block), blocks.dtype),
            pltpu.VMEM((2, 16, 2, block, block), blocks.dtype),
            pltpu.VMEM((2, 4, 2, block, block), jnp.float32),
            pltpu.VMEM((4, 2, block, block), blocks.dtype),
            pltpu.VMEM((band, block // 2, block), blocks.dtype),
            pltpu.VMEM((8, block), jnp.int32),
            dma((16,)), dma((6, 16)), dma((4, 16)), dma((2, 8, 2, 2)), dma((2, 16, 2)), dma((8,)), dma((8,)),
        ],
        compiler_params=pltpu.CompilerParams(
            collective_id=0, has_side_effects=True, vmem_limit_bytes=60 * 1024 * 1024
        ),
    )(columns, blocks[0])
    return result[None].astype(jnp.float32)


def from_behind(value, axis, steps):
    count = lax.axis_size(axis)
    pairs = [(source, (source + steps) % count) for source in range(count)]
    return lax.ppermute(value, axis, pairs)


def live_table(columns):
    nrows, band_width = columns.shape
    half_band = band_width // 2
    row_ids = jnp.arange(nrows, dtype=jnp.int32)
    target = (
        row_ids[:, None] + jnp.arange(band_width, dtype=jnp.int32)[None, :] - half_band
    ) % nrows
    return jnp.any(columns[:, None, :] == target[:, :, None], axis=2)


def slot_shift(piece, delta):
    band_width = piece.shape[1]
    if delta >= 0:
        return jnp.concatenate([piece[:, delta:], jnp.zeros_like(piece[:, :delta])], axis=1)
    return jnp.concatenate(
        [jnp.zeros_like(piece[:, :-delta]), piece[:, : band_width + delta]], axis=1
    )


def fetch_band(row_slab, below, above, block_rows, second):
    band_width = row_slab.shape[1]
    pieces = []
    for offset in range(-below, above + 1):
        if offset == 0:
            pieces.append(row_slab)
            continue
        trimmed = (abs(offset) - 1) * block_rows + 1
        if offset > 0:
            outgoing = row_slab[:, : band_width - trimmed]
        else:
            outgoing = row_slab[:, trimmed:]
        if second:
            incoming = from_behind(outgoing, "rows", -offset)
        else:
            incoming = from_behind(outgoing, "rows", -offset)
        filler = jnp.zeros_like(row_slab[:, :trimmed])
        if offset > 0:
            pieces.append(jnp.concatenate([incoming, filler], axis=1))
        else:
            pieces.append(jnp.concatenate([filler, incoming], axis=1))
    return jnp.concatenate(pieces, axis=0)


def merge_groups(totals):
    rounded = lax.optimization_barrier(totals.astype(jnp.bfloat16))
    return jnp.sum(rounded.astype(jnp.float32), axis=0)


def dense_terms(left, window, window_base, groups):
    block_rows, band_width, block_size, inner_width = left.shape
    out_width = window.shape[3]
    half_band = band_width // 2
    group_width = inner_width // groups
    stacked = jnp.stack(
        [
            slot_shift(
                window[window_base + offset : window_base + offset + block_rows], half_band - offset
            )
            for offset in range(band_width)
        ],
        axis=1,
    )
    left_groups = left.reshape(block_rows, band_width, block_size, groups, group_width)
    right_groups = stacked.reshape(
        block_rows, band_width, band_width, groups, group_width, out_width
    )
    totals = jnp.einsum(
        "ramcq,rascqn->crsmn", left_groups, right_groups, preferred_element_type=jnp.float32
    )
    return merge_groups(totals)


def band_terms(left, window, window_base, groups):
    return dense_terms(left, window, window_base, groups)


def per_device(blocks, columns):
    block_rows, band_width, block_size, _ = blocks.shape
    half_band = band_width // 2
    inner_count = lax.axis_size("inner")
    slab_width = block_size // inner_count
    inner_index = lax.axis_index("inner")
    row_owner = lax.axis_index("rows")
    live_own = lax.dynamic_slice_in_dim(live_table(columns), row_owner * block_rows, block_rows, 0)
    live_slots = live_own[:, :, None, None]
    masked = jnp.where(live_slots, blocks, jnp.zeros_like(blocks))
    below = -(-half_band // block_rows)
    above = -(-(half_band - 1) // block_rows)
    window_base = below * block_rows - half_band
    row_slab = lax.dynamic_slice_in_dim(masked, inner_index * slab_width, slab_width, 3)
    window = fetch_band(row_slab, below, above, block_rows, False)
    square = band_terms(masked, window, window_base, inner_count)
    square = jnp.where(live_slots, square, jnp.float32(0.0)).astype(jnp.bfloat16)
    second_window = fetch_band(square, below, above, block_rows, True)
    cubed = band_terms(masked, second_window, window_base, inner_count)
    cubed = jnp.where(live_slots, cubed, jnp.float32(0.0))
    column_slabs = 3.0 * square.astype(jnp.float32) - 2.0 * cubed
    return lax.all_to_all(
        column_slabs.astype(jnp.bfloat16), "inner", split_axis=2, concat_axis=3, tiled=True
    ).astype(column_slabs.dtype)


def solution(mesh):
    in_specs = (P("rows", None, None, None), P())
    out_specs = P("rows", None, "inner", None)

    def step(blocks, columns):
        plain = mesh.shape["rows"] == 16 and mesh.shape["inner"] == 2
        if plain and blocks.shape[:2] == (16, 16) and blocks.shape[2] % 256 == 0:
            chosen = on_grid
        else:
            chosen = per_device
        return jax.shard_map(chosen, mesh=mesh, in_specs=in_specs, out_specs=out_specs, check_vma=False)(
            blocks, columns
        )

    return step
```

```python
import functools

import jax
import jax.numpy as jnp
from jax import lax
from jax.experimental import pallas as pl
from jax.experimental.pallas import tpu as pltpu
from jax.sharding import PartitionSpec as P

MESH = pl.DeviceIdType.MESH

WINDOW = 3
EXTRA = ((1, 0),)
GROUP = ((0, 0), (1, 0), (0, 1), (1, 1))
ORDER = (
    ("x", 1, 1, 0, 0), ("x", 1, 1, 0, 1), ("l", 1, 0, 0, 0, 0), ("n", 1, 0), ("l", 1, 0, 0, 0, 1),
("l", 2, 0, 1, 0, 0), ("n", 0, 1), ("x", 0, 0, 0, 0), ("l", 1, 1, 0, 0, 0), ("l", 1, 1, 0, 0, 1),
("l", 2, 0, 1, 0, 1), ("x", 0, 0, 0, 1), ("p", 4, 0), ("l", 3, 0, 0, 0, 0), ("n", 3, 0), ("x", 1, 0, 0, 0),
("l", 2, 0, 0, 0, 0), ("n", 2, 0), ("l", 1, 0, 1, 0, 0), ("p", 5, 0), ("l", 3, 0, 0, 0, 1),
("x", 1, 0, 0, 1), ("n", 1, 1), ("l", 1, 0, 1, 0, 1), ("l", 2, 0, 0, 0, 1), ("n", 3, 1), ("n", 2, 1),
("l", 3, 0, 1, 0, 0), ("x", 1, 0, 1, 0), ("x", 1, 0, 1, 1), ("l", 1, 1, 1, 0, 0), ("p", 7, 0),
("l", 2, 1, 1, 0, 0), ("p", 6, 0), ("l", 3, 0, 1, 0, 1), ("l", 1, 1, 1, 0, 1), ("l", 2, 1, 1, 0, 1),
("s", 0, 0, 0), ("l", 3, 1, 0, 0, 0), ("p", 4, 1), ("p", 5, 1), ("l", 2, 1, 0, 0, 0), ("m", 1, 0, 0, 4),
("m", 2, 0, 0, 4), ("s", 1, 0, 4), ("l", 3, 1, 0, 0, 1), ("p", 7, 1), ("l", 2, 1, 0, 0, 1),
("m", 3, 0, 0, 4), ("p", 6, 1), ("s", 0, 1, 0), ("l", 3, 1, 1, 0, 0), ("m", 1, 1, 0, 4), ("s", 1, 1, 4),
("m", 2, 1, 0, 4), ("l", 3, 1, 1, 0, 1), ("m", 3, 1, 0, 4), ("s", 2, 0, 4), ("q", 4, 0), ("s", 3, 0, 4),
("q", 5, 0), ("c", 0, 0, 1, 4), ("s", 2, 1, 4), ("q", 6, 0), ("s", 3, 1, 4), ("c", 0, 8, 1, 2),
("c", 0, 4, 1, 2), ("c", 0, 12, 1, 2), ("c", 0, 10, 1, 2), ("q", 7, 0), ("c", 0, 6, 8, 2),
("c", 0, 7, 8, 2), ("e", 0), ("q", 4, 1), ("q", 5, 1), ("c", 1, 0, 1, 4), ("c", 1, 8, 1, 2),
("c", 1, 4, 1, 2), ("c", 1, 12, 1, 2), ("q", 6, 1), ("c", 1, 10, 1, 2), ("c", 1, 6, 8, 2), ("q", 7, 1),
("c", 1, 7, 8, 2), ("e", 1),
)


def grid_kernel(columns, raw, out, left, panels, acc, pure, final, keep_lanes, load_sem,
                left_send, left_recv, panel_send, panel_recv, end_send, end_recv):
    band, block = raw.shape[0], raw.shape[1]
    slab = block // 2
    rank, y = lax.axis_index("rows"), lax.axis_index("inner")
    core, x, low, high = rank % 2, (rank // 2) % 2, (rank // 4) % 2, rank // 8
    other_y = 1 - y

    def wrap(value):
        return lax.rem(value, band)

    def flip(bit, by):
        return 1 - bit if by else bit

    def row_at(core_by, x_by, low_by, high_by):
        return 8 * flip(high, high_by) + 4 * flip(low, low_by) + 2 * flip(x, x_by) + flip(core, core_by)

    group_rows = [row_at(0, x_by, 0, high_by) for x_by, high_by in GROUP]
    at_y = {"rows": rank, "inner": other_y}
    at_core = {"rows": row_at(1, 0, 0, 0), "inner": y}
    at_x = {"rows": group_rows[1], "inner": y}
    at_near = {"rows": row_at(0, 0, 1, 0), "inner": y}
    at_far = {"rows": group_rows[2], "inner": y}
    at_xy = {"rows": group_rows[1], "inner": other_y}
    at_far_y = {"rows": group_rows[2], "inner": other_y}
    at_far_x = {"rows": group_rows[3], "inner": y}
    at_far_xy = {"rows": group_rows[3], "inner": other_y}
    everyone = (at_y, at_core, at_x, at_near, at_far, at_xy, at_far_y, at_far_x, at_far_xy)

    barrier = pltpu.get_barrier_semaphore()
    for device in everyone:
        pl.semaphore_signal(barrier, inc=1, device_id=device, device_id_type=MESH)

    loads = []
    for slot in range(band):
        column = wrap(rank + slot + band // 2)
        load = pltpu.make_async_copy(raw.at[slot], left.at[0, column], load_sem.at[slot])
        load.start()
        loads.append(load)

    sent = []

    def remote(source, target, send_sem, recv_sem, device):
        return pltpu.make_async_remote_copy(
            src_ref=source, dst_ref=target, send_sem=send_sem, recv_sem=recv_sem, device_id=device, device_id_type=MESH
        )

    def only(wanted, act):
        if wanted is None:
            act()
        else:
            pl.when(wanted)(act)

    def go(copy, wanted=None):
        only(wanted, copy.start)
        sent.append((copy, wanted))

    def column_of(high_by, x_by, y_by, part):
        return 2 * (4 * flip(high, high_by) + 2 * flip(x, x_by) + flip(y, y_by)) + part

    mine = column_of(0, 0, 0, 0)

    def is_read(row, inner_row, first, count):
        s = wrap(first - row + band + band // 2)
        a = wrap(inner_row - row + band + band // 2)
        return (s + count > band) | ((a - s <= band // 2 - 1 + count) & (s - a <= band // 2 - 1))

    def read_by(which, at, flow, y_by):
        row = group_rows[which]
        if flow == "y":
            return is_read(row, at, column_of(0, 0, 1, 0), 2)
        if y_by:
            return is_read(row, at, column_of(0, 1, 0, 0), 2)
        return is_read(row, at, 2 * (4 * high + 2 * (1 - x)), 4)

    def is_live(row, slot):
        target = wrap(row + slot + band // 2)
        found = columns[row, 0] == target
        for at in range(1, columns.shape[1]):
            found = found | (columns[row, at] == target)
        return jnp.where(found, 1, 0)

    def send_left(flow, source, target, device, at, wanted):
        go(remote(left.at[source, at], left.at[target, at], left_send.at[flow, at], left_recv.at[target, at], device), wanted)

    def to_x(source, high_by, x_by, y_by, part):
        at = column_of(high_by, x_by, y_by, part)
        panel = (high_by, x_by, y_by) == (0, 1, 0)
        wanted = None if panel else read_by(source, at, "x", y_by)
        send_left(1 if source == 0 else 2, source, source + 1, at_x, at, wanted)

    def by_x(which, high_by, x_by, y_by):
        return y_by == 0 or (which == 1 and (high_by, 1 - x_by) in EXTRA)

    done = set()

    def take(which, high_by, x_by, y_by, part):
        key = ("left", which, high_by, x_by, y_by, part)
        if key in done:
            return
        done.add(key)
        at = column_of(high_by, x_by, y_by, part)
        ref = left.at[which, at]
        copy = remote(ref, ref, left_send.at[0, at], left_recv.at[which, at], at_y)
        wanted = None
        if y_by:
            wanted = is_read(group_rows[which], at, mine, 2)
        elif which != 2 and (high_by, x_by) != (0, 0):
            wanted = is_read(group_rows[which], at, 2 * (4 * high + 2 * x), 4)
        only(wanted, copy.wait_recv)
        if y_by:
            return
        if (high_by, x_by) == (0, 0):
            panels[0, which, part] = left[which, mine + part]
        if which == 2 and fars:
            to_far(*fars.pop(0))
        if which == 2:
            to_x(2, high_by, x_by, 0, part)
        if not (which == 1 and (high_by, 1 - x_by) in EXTRA):
            send_left(2 + which, which, which, at_y, at, read_by(which, at, "y", 0))

    def send_panel(product, source, target, part, device):
        own = product == 0 and source < 4
        ref = left.at[source, mine + part] if own else panels.at[product, source, part]
        go(remote(ref, panels.at[product, target, part], panel_send.at[product, source, target // 8, part],
                  panel_recv.at[product, target, part], device))

    def share(product, which, part):
        send_panel(product, which, 4 + which, part, at_near)
        send_panel(product, which, 8 + which, part, at_core)

    def take_panel(product, source, part):
        key = ("panel", product, source, part)
        if key in done:
            return
        done.add(key)
        ref = panels.at[product, source, part]
        remote(ref, ref, panel_send.at[product, 0, 0, 0], panel_recv.at[product, source, part], at_core).wait_recv()
        if source < 8:
            send_panel(product, source, 8 + source, part, at_core)

    def own_panel(which, part):
        if which:
            take(which, 0, 0, 0, part)
        else:
            panels[0, which, part] = left[which, mine + part]
        share(0, which, part)

    def apart(a, b):
        return a + b - 2 * a * b

    def source_of(row):
        return (8 * apart(row % 2, core) + 4 * apart((row // 4) % 2, low)
                + 2 * apart(row // 8, high) + apart((row // 2) % 2, x))

    def row_of(source):
        return (8 * apart((source // 2) % 2, high) + 4 * apart((source // 4) % 2, low)
                + 2 * apart(source % 2, x) + apart(source // 8, core))

    def mac(product, which, part, terms):
        row = group_rows[which]
        total = None
        for inner_row, source in terms:
            valid = is_read(row, inner_row, mine + part, 1)
            term = jnp.dot(left[which, inner_row], panels[product, source, part], preferred_element_type=jnp.float32)
            term = jnp.where(valid, term, 0.0)
            total = term if total is None else total + term
        acc[product, which, part] += total

    def take_row(which):
        for high_by in range(2 if which else 0):
            for x_by in range(2):
                for y_by in range(2):
                    for part in range(2):
                        take(which, high_by, x_by, y_by, part)

    def square_macs(which, part, first, count):
        for high_by in range(first // 4, (first + count) // 4):
            for x_by in range(2):
                for y_by in range(2):
                    for at in range(2):
                        if which:
                            take(which, high_by, x_by, y_by, at)
        for source in range(1, 4):
            take(source, 0, 0, 0, part)
        for source in range(4, 16):
            take_panel(0, source, part)

        def body(n, carry):
            high_by, x_by, y_by = n // 4, lax.rem(n // 2, 2), lax.rem(n, 2)
            inner_row = 2 * (4 * apart(high, high_by) + 2 * apart(x, x_by) + apart(y, y_by))
            mac(0, which, part, [(inner_row + step, source_of(inner_row + step)) for step in range(2)])
            return carry

        lax.fori_loop(first, first + count, body, 0)
        assert (which, part) not in done
        done.add((which, part, first + count))

    def cube_macs(part, first, stride, count):
        for which in range(4):
            take_row(which)
        for n in range(count):
            source = first + n * stride
            done.add(("cube", source, part))
            if source < 4:
                assert (source, part) in done
            else:
                take_panel(1, source, part)

        def body(n, carry):
            sources = [first + (2 * n + step) * stride for step in range(2)]
            for which in range(4):
                mac(1, which, part, [(row_of(source), source) for source in sources])
            return carry

        lax.fori_loop(0, count // 2, body, 0)

    def masked(product, which, part):
        keep = keep_lanes[2 * which + part : 2 * which + part + 1] > 0
        return jnp.where(keep, acc[product, which, part], 0.0)

    def square(which, part, first):
        assert first == 0 or (which, part, first) in done
        square_macs(which, part, first, 8 - first)
        done.add((which, part))
        panels[1, which, part] = masked(0, which, part).astype(panels.dtype)
        share(1, which, part)

    def mask_slot(slot, carry):
        column = wrap(rank + slot + band // 2)
        keep = jnp.full((1, block), is_live(rank, slot)) > 0
        value = left[0, column]
        left[0, column] = jnp.where(keep, value, jnp.zeros_like(value))
        return carry

    for load in loads:
        load.wait()
    lax.fori_loop(0, band, mask_slot, 0)
    pl.semaphore_wait(barrier, len(everyone))

    def to_far(high_by, x_by, part):
        at = column_of(high_by, x_by, 0, part)
        send_left(0, 0, 2, at_far, at, None)

    fars = [(high_by, x_by, part) for high_by, x_by in ((1, 1), (1, 0), (0, 1), (0, 0)) for part in range(2)]
    for _ in range(WINDOW):
        to_far(*fars.pop(0))
    for part in range(2):
        to_x(0, 0, 1, 0, part)
    own_panel(0, 0)
    for which in range(4):
        for part in range(2):
            row = group_rows[which]
            live = is_live(row, wrap(mine + part - row + band + band // 2))
            at = 2 * which + part
            keep_lanes[at : at + 1] = jnp.full((1, block), live)
    acc[...] = jnp.zeros_like(acc)

    here = pl.ds(pl.multiple_of(y * slab, slab), slab)
    there = pl.ds(pl.multiple_of(other_y * slab, slab), slab)
    ends = {0: ((1, at_y),), 1: ((1, at_xy), (0, at_x)), 2: ((1, at_far_y), (0, at_far)), 3: ((1, at_far_xy), (0, at_far_x))}

    def finish(part):
        assert all(("cube", source, part) in done for source in range(16))
        for which in (3, 2, 1, 0):
            total = 3.0 * panels[1, which, part].astype(jnp.float32) - 2.0 * masked(1, which, part)
            pure[which, part] = total.astype(pure.dtype)
            for half, device in ends[which]:
                at = 2 * which + half
                rows = there if half else here
                go(remote(pure.at[which, part, rows], final.at[mine + part], end_send.at[at, part],
                          end_recv.at[at, part], device))

    acts = {"x": lambda a, b, w, t: to_x(0, a, b, w, t), "l": take, "n": own_panel,
            "p": lambda s, t: take_panel(0, s, t), "q": lambda s, t: take_panel(1, s, t),
            "m": square_macs, "s": square, "c": cube_macs, "e": finish}
    for name, *numbers in ORDER:
        acts[name](*numbers)

    def place(value, column):
        out[wrap(column - rank + band + band // 2)] = value

    for part in range(2):
        place(pure[0, part, here], mine + part)
        for which in range(4):
            for half, _ in ends[which]:
                x_by, high_by = GROUP[which]
                at = column_of(high_by, x_by, half, part)
                ref = final.at[at]
                remote(ref, ref, end_send.at[0, 0], end_recv.at[2 * which + half, part], at_y).wait_recv()
                place(final[at], at)
    for copy, wanted in sent:
        only(wanted, copy.wait_send)


def on_grid(blocks, columns):
    _, band, block, _ = blocks.shape
    vmem = pl.BlockSpec(memory_space=pltpu.VMEM)
    dma = pltpu.SemaphoreType.DMA
    result = pl.pallas_call(
        grid_kernel,
        out_shape=jax.ShapeDtypeStruct((band, block // 2, block), blocks.dtype),
        in_specs=[pl.BlockSpec(memory_space=pltpu.SMEM), pl.BlockSpec(memory_space=pl.ANY)],
        out_specs=vmem,
        scratch_shapes=[
            pltpu.VMEM((4, band, block, block), blocks.dtype),
            pltpu.VMEM((2, 16, 2, block, block), blocks.dtype),
            pltpu.VMEM((2, 4, 2, block, block), jnp.float32),
            pltpu.VMEM((4, 2, block, block), blocks.dtype),
            pltpu.VMEM((band, block // 2, block), blocks.dtype),
            pltpu.VMEM((8, block), jnp.int32),
            dma((16,)), dma((6, 16)), dma((4, 16)), dma((2, 8, 2, 2)), dma((2, 16, 2)), dma((8, 2)), dma((8, 2)),
        ],
        compiler_params=pltpu.CompilerParams(
            collective_id=0, has_side_effects=True, vmem_limit_bytes=60 * 1024 * 1024
        ),
    )(columns, blocks[0])
    return result[None].astype(jnp.float32)


def from_behind(value, axis, steps):
    count = lax.axis_size(axis)
    pairs = [(source, (source + steps) % count) for source in range(count)]
    return lax.ppermute(value, axis, pairs)


def live_table(columns):
    nrows, band_width = columns.shape
    half_band = band_width // 2
    row_ids = jnp.arange(nrows, dtype=jnp.int32)
    target = (
        row_ids[:, None] + jnp.arange(band_width, dtype=jnp.int32)[None, :] - half_band
    ) % nrows
    return jnp.any(columns[:, None, :] == target[:, :, None], axis=2)


def slot_shift(piece, delta):
    band_width = piece.shape[1]
    if delta >= 0:
        return jnp.concatenate([piece[:, delta:], jnp.zeros_like(piece[:, :delta])], axis=1)
    return jnp.concatenate(
        [jnp.zeros_like(piece[:, :-delta]), piece[:, : band_width + delta]], axis=1
    )


def fetch_band(row_slab, below, above, block_rows, second):
    band_width = row_slab.shape[1]
    pieces = []
    for offset in range(-below, above + 1):
        if offset == 0:
            pieces.append(row_slab)
            continue
        trimmed = (abs(offset) - 1) * block_rows + 1
        if offset > 0:
            outgoing = row_slab[:, : band_width - trimmed]
        else:
            outgoing = row_slab[:, trimmed:]
        if second:
            incoming = from_behind(outgoing, "rows", -offset)
        else:
            incoming = from_behind(outgoing, "rows", -offset)
        filler = jnp.zeros_like(row_slab[:, :trimmed])
        if offset > 0:
            pieces.append(jnp.concatenate([incoming, filler], axis=1))
        else:
            pieces.append(jnp.concatenate([filler, incoming], axis=1))
    return jnp.concatenate(pieces, axis=0)


def merge_groups(totals):
    rounded = lax.optimization_barrier(totals.astype(jnp.bfloat16))
    return jnp.sum(rounded.astype(jnp.float32), axis=0)


def dense_terms(left, window, window_base, groups):
    block_rows, band_width, block_size, inner_width = left.shape
    out_width = window.shape[3]
    half_band = band_width // 2
    group_width = inner_width // groups
    stacked = jnp.stack(
        [
            slot_shift(
                window[window_base + offset : window_base + offset + block_rows], half_band - offset
            )
            for offset in range(band_width)
        ],
        axis=1,
    )
    left_groups = left.reshape(block_rows, band_width, block_size, groups, group_width)
    right_groups = stacked.reshape(
        block_rows, band_width, band_width, groups, group_width, out_width
    )
    totals = jnp.einsum(
        "ramcq,rascqn->crsmn", left_groups, right_groups, preferred_element_type=jnp.float32
    )
    return merge_groups(totals)


def band_terms(left, window, window_base, groups):
    return dense_terms(left, window, window_base, groups)


def per_device(blocks, columns):
    block_rows, band_width, block_size, _ = blocks.shape
    half_band = band_width // 2
    inner_count = lax.axis_size("inner")
    slab_width = block_size // inner_count
    inner_index = lax.axis_index("inner")
    row_owner = lax.axis_index("rows")
    live_own = lax.dynamic_slice_in_dim(live_table(columns), row_owner * block_rows, block_rows, 0)
    live_slots = live_own[:, :, None, None]
    masked = jnp.where(live_slots, blocks, jnp.zeros_like(blocks))
    below = -(-half_band // block_rows)
    above = -(-(half_band - 1) // block_rows)
    window_base = below * block_rows - half_band
    row_slab = lax.dynamic_slice_in_dim(masked, inner_index * slab_width, slab_width, 3)
    window = fetch_band(row_slab, below, above, block_rows, False)
    square = band_terms(masked, window, window_base, inner_count)
    square = jnp.where(live_slots, square, jnp.float32(0.0)).astype(jnp.bfloat16)
    second_window = fetch_band(square, below, above, block_rows, True)
    cubed = band_terms(masked, second_window, window_base, inner_count)
    cubed = jnp.where(live_slots, cubed, jnp.float32(0.0))
    column_slabs = 3.0 * square.astype(jnp.float32) - 2.0 * cubed
    return lax.all_to_all(
        column_slabs.astype(jnp.bfloat16), "inner", split_axis=2, concat_axis=3, tiled=True
    ).astype(column_slabs.dtype)


def solution(mesh):
    in_specs = (P("rows", None, None, None), P())
    out_specs = P("rows", None, "inner", None)

    def step(blocks, columns):
        plain = mesh.shape["rows"] == 16 and mesh.shape["inner"] == 2
        if plain and blocks.shape[:2] == (16, 16) and blocks.shape[2] % 256 == 0:
            chosen = on_grid
        else:
            chosen = per_device
        return jax.shard_map(chosen, mesh=mesh, in_specs=in_specs, out_specs=out_specs, check_vma=False)(
            blocks, columns
        )

    return step
```

```python
import functools

import jax
import jax.numpy as jnp
from jax import lax
from jax.experimental import pallas as pl
from jax.experimental.pallas import tpu as pltpu
from jax.sharding import PartitionSpec as P

MESH = pl.DeviceIdType.MESH

WINDOW = 2
DIAGONAL = ((1, 0, 1),)
EXTRA = ((1, 0),)
GROUP = ((0, 0), (1, 0), (0, 1), (1, 1))
ORDER = (
    ("x", 1, 1, 0, 0), ("x", 1, 1, 0, 1), ("l", 1, 0, 0, 0, 0), ("n", 1, 0), ("l", 1, 0, 0, 0, 1),
("l", 2, 0, 1, 0, 0), ("n", 0, 1), ("x", 0, 0, 0, 0), ("l", 1, 1, 0, 0, 0), ("l", 1, 1, 0, 0, 1),
("l", 2, 0, 1, 0, 1), ("x", 0, 0, 0, 1), ("p", 4, 0), ("l", 3, 0, 0, 0, 0), ("n", 3, 0), ("x", 1, 0, 0, 0),
("l", 2, 0, 0, 0, 0), ("n", 2, 0), ("l", 1, 0, 1, 0, 0), ("p", 5, 0), ("l", 3, 0, 0, 0, 1),
("x", 1, 0, 0, 1), ("n", 1, 1), ("l", 1, 0, 1, 0, 1), ("l", 2, 0, 0, 0, 1), ("n", 3, 1), ("n", 2, 1),
("l", 3, 0, 1, 0, 0), ("x", 1, 0, 1, 0), ("x", 1, 0, 1, 1), ("l", 1, 1, 1, 0, 0), ("p", 7, 0),
("l", 2, 1, 1, 0, 0), ("p", 6, 0), ("l", 3, 0, 1, 0, 1), ("l", 1, 1, 1, 0, 1), ("l", 2, 1, 1, 0, 1),
("s", 0, 0, 0), ("l", 3, 1, 0, 0, 0), ("p", 4, 1), ("p", 5, 1), ("l", 2, 1, 0, 0, 0), ("m", 1, 0, 0, 4),
("m", 2, 0, 0, 4), ("s", 1, 0, 4), ("l", 3, 1, 0, 0, 1), ("p", 7, 1), ("l", 2, 1, 0, 0, 1),
("m", 3, 0, 0, 4), ("p", 6, 1), ("s", 0, 1, 0), ("l", 3, 1, 1, 0, 0), ("m", 1, 1, 0, 4), ("s", 1, 1, 4),
("m", 2, 1, 0, 4), ("l", 3, 1, 1, 0, 1), ("m", 3, 1, 0, 4), ("s", 2, 0, 4), ("q", 4, 0), ("s", 3, 0, 4),
("q", 5, 0), ("c", 0, 0, 1, 4), ("s", 2, 1, 4), ("q", 6, 0), ("s", 3, 1, 4), ("c", 0, 8, 1, 2),
("c", 0, 4, 1, 2), ("c", 0, 12, 1, 2), ("c", 0, 10, 1, 2), ("q", 7, 0), ("c", 0, 6, 8, 2),
("c", 0, 7, 8, 2), ("e", 0), ("q", 4, 1), ("q", 5, 1), ("c", 1, 0, 1, 4), ("c", 1, 8, 1, 2),
("c", 1, 4, 1, 2), ("c", 1, 12, 1, 2), ("q", 6, 1), ("c", 1, 10, 1, 2), ("c", 1, 6, 8, 2), ("q", 7, 1),
("c", 1, 7, 8, 2), ("e", 1),
)


def grid_kernel(columns, raw, out, left, panels, acc, pure, final, keep_lanes, load_sem,
                left_send, left_recv, panel_send, panel_recv, end_send, end_recv):
    band, block = raw.shape[0], raw.shape[1]
    slab = block // 2
    rank, y = lax.axis_index("rows"), lax.axis_index("inner")
    core, x, low, high = rank % 2, (rank // 2) % 2, (rank // 4) % 2, rank // 8
    other_y = 1 - y

    def wrap(value):
        return lax.rem(value, band)

    def flip(bit, by):
        return 1 - bit if by else bit

    def row_at(core_by, x_by, low_by, high_by):
        return 8 * flip(high, high_by) + 4 * flip(low, low_by) + 2 * flip(x, x_by) + flip(core, core_by)

    group_rows = [row_at(0, x_by, 0, high_by) for x_by, high_by in GROUP]
    at_y = {"rows": rank, "inner": other_y}
    at_core = {"rows": row_at(1, 0, 0, 0), "inner": y}
    at_x = {"rows": group_rows[1], "inner": y}
    at_near = {"rows": row_at(0, 0, 1, 0), "inner": y}
    at_far = {"rows": group_rows[2], "inner": y}
    at_xy = {"rows": group_rows[1], "inner": other_y}
    at_far_y = {"rows": group_rows[2], "inner": other_y}
    at_far_x = {"rows": group_rows[3], "inner": y}
    at_far_xy = {"rows": group_rows[3], "inner": other_y}
    everyone = (at_y, at_core, at_x, at_near, at_far, at_xy, at_far_y, at_far_x, at_far_xy)

    barrier = pltpu.get_barrier_semaphore()
    for device in everyone:
        pl.semaphore_signal(barrier, inc=1, device_id=device, device_id_type=MESH)

    loads = []
    for slot in range(band):
        column = wrap(rank + slot + band // 2)
        load = pltpu.make_async_copy(raw.at[slot], left.at[0, column], load_sem.at[slot])
        load.start()
        loads.append(load)

    sent = []

    def remote(source, target, send_sem, recv_sem, device):
        return pltpu.make_async_remote_copy(
            src_ref=source, dst_ref=target, send_sem=send_sem, recv_sem=recv_sem, device_id=device, device_id_type=MESH
        )

    def only(wanted, act):
        if wanted is None:
            act()
        else:
            pl.when(wanted)(act)

    def go(copy, wanted=None):
        only(wanted, copy.start)
        sent.append((copy, wanted))

    def column_of(high_by, x_by, y_by, part):
        return 2 * (4 * flip(high, high_by) + 2 * flip(x, x_by) + flip(y, y_by)) + part

    mine = column_of(0, 0, 0, 0)

    def is_read(row, inner_row, first, count):
        s = wrap(first - row + band + band // 2)
        a = wrap(inner_row - row + band + band // 2)
        return (s + count > band) | ((a - s <= band // 2 - 1 + count) & (s - a <= band // 2 - 1))

    def read_by(which, at, flow, y_by):
        row = group_rows[which]
        if flow == "y":
            return is_read(row, at, column_of(0, 0, 1, 0), 2)
        if y_by:
            return is_read(row, at, column_of(0, 1, 0, 0), 2)
        return is_read(row, at, 2 * (4 * high + 2 * (1 - x)), 4)

    def is_live(row, slot):
        target = wrap(row + slot + band // 2)
        found = columns[row, 0] == target
        for at in range(1, columns.shape[1]):
            found = found | (columns[row, at] == target)
        return jnp.where(found, 1, 0)

    def send_left(flow, source, target, device, at, wanted):
        go(remote(left.at[source, at], left.at[target, at], left_send.at[flow, at], left_recv.at[target, at], device), wanted)

    def to_x(source, high_by, x_by, y_by, part):
        at = column_of(high_by, x_by, y_by, part)
        panel = (high_by, x_by, y_by) == (0, 1, 0)
        wanted = None if panel else read_by(source, at, "x", y_by)
        send_left(1 if source == 0 else 2, source, source + 1, at_x, at, wanted)

    def by_x(which, high_by, x_by, y_by):
        return y_by == 0 or (which == 1 and (high_by, 1 - x_by) in EXTRA)

    done = set()

    def take(which, high_by, x_by, y_by, part):
        key = ("left", which, high_by, x_by, y_by, part)
        if key in done:
            return
        done.add(key)
        at = column_of(high_by, x_by, y_by, part)
        ref = left.at[which, at]
        copy = remote(ref, ref, left_send.at[0, at], left_recv.at[which, at], at_y)
        wanted = None
        if y_by:
            wanted = is_read(group_rows[which], at, mine, 2)
        elif which != 2 and (high_by, x_by) != (0, 0):
            wanted = is_read(group_rows[which], at, 2 * (4 * high + 2 * x), 4)
        only(wanted, copy.wait_recv)
        if y_by:
            return
        if (high_by, x_by) == (0, 0):
            panels[0, which, part] = left[which, mine + part]
        if which == 2 and fars:
            to_far(*fars.pop(0))
        if which == 2:
            to_x(2, high_by, x_by, 0, part)
            if (high_by, x_by, part) in DIAGONAL:
                wanted = is_read(group_rows[2], at, column_of(0, 1, 1, 0), 2)
                send_left(6, 2, 3, at_xy, at, wanted)
        if not (which == 1 and (high_by, 1 - x_by) in EXTRA or which == 3 and (high_by, 1 - x_by, part) in DIAGONAL):
            send_left(2 + which, which, which, at_y, at, read_by(which, at, "y", 0))

    def send_panel(product, source, target, part, device):
        own = product == 0 and source < 4
        ref = left.at[source, mine + part] if own else panels.at[product, source, part]
        go(remote(ref, panels.at[product, target, part], panel_send.at[product, source, target // 8, part],
                  panel_recv.at[product, target, part], device))

    def share(product, which, part):
        send_panel(product, which, 4 + which, part, at_near)
        send_panel(product, which, 8 + which, part, at_core)

    def take_panel(product, source, part):
        key = ("panel", product, source, part)
        if key in done:
            return
        done.add(key)
        ref = panels.at[product, source, part]
        remote(ref, ref, panel_send.at[product, 0, 0, 0], panel_recv.at[product, source, part], at_core).wait_recv()
        if source < 8:
            send_panel(product, source, 8 + source, part, at_core)

    def own_panel(which, part):
        if which:
            take(which, 0, 0, 0, part)
        else:
            panels[0, which, part] = left[which, mine + part]
        share(0, which, part)

    def apart(a, b):
        return a + b - 2 * a * b

    def source_of(row):
        return (8 * apart(row % 2, core) + 4 * apart((row // 4) % 2, low)
                + 2 * apart(row // 8, high) + apart((row // 2) % 2, x))

    def row_of(source):
        return (8 * apart((source // 2) % 2, high) + 4 * apart((source // 4) % 2, low)
                + 2 * apart(source % 2, x) + apart(source // 8, core))

    def mac(product, which, part, terms):
        row = group_rows[which]
        total = None
        for inner_row, source in terms:
            valid = is_read(row, inner_row, mine + part, 1)
            term = jnp.dot(left[which, inner_row], panels[product, source, part], preferred_element_type=jnp.float32)
            term = jnp.where(valid, term, 0.0)
            total = term if total is None else total + term
        acc[product, which, part] += total

    def take_row(which):
        for high_by in range(2 if which else 0):
            for x_by in range(2):
                for y_by in range(2):
                    for part in range(2):
                        take(which, high_by, x_by, y_by, part)

    def square_macs(which, part, first, count):
        for high_by in range(first // 4, (first + count) // 4):
            for x_by in range(2):
                for y_by in range(2):
                    for at in range(2):
                        if which:
                            take(which, high_by, x_by, y_by, at)
        for source in range(1, 4):
            take(source, 0, 0, 0, part)
        for source in range(4, 16):
            take_panel(0, source, part)

        def body(n, carry):
            high_by, x_by, y_by = n // 4, lax.rem(n // 2, 2), lax.rem(n, 2)
            inner_row = 2 * (4 * apart(high, high_by) + 2 * apart(x, x_by) + apart(y, y_by))
            mac(0, which, part, [(inner_row + step, source_of(inner_row + step)) for step in range(2)])
            return carry

        lax.fori_loop(first, first + count, body, 0)
        assert (which, part) not in done
        done.add((which, part, first + count))

    def cube_macs(part, first, stride, count):
        for which in range(4):
            take_row(which)
        for n in range(count):
            source = first + n * stride
            done.add(("cube", source, part))
            if source < 4:
                assert (source, part) in done
            else:
                take_panel(1, source, part)

        def body(n, carry):
            sources = [first + (2 * n + step) * stride for step in range(2)]
            for which in range(4):
                mac(1, which, part, [(row_of(source), source) for source in sources])
            return carry

        lax.fori_loop(0, count // 2, body, 0)

    def masked(product, which, part):
        keep = keep_lanes[2 * which + part : 2 * which + part + 1] > 0
        return jnp.where(keep, acc[product, which, part], 0.0)

    def square(which, part, first):
        assert first == 0 or (which, part, first) in done
        square_macs(which, part, first, 8 - first)
        done.add((which, part))
        panels[1, which, part] = masked(0, which, part).astype(panels.dtype)
        share(1, which, part)

    def mask(column):
        row_slot = wrap(column - rank + band + band // 2)
        keep = jnp.full((1, block), is_live(rank, row_slot)) > 0
        value = left[0, column]
        left[0, column] = jnp.where(keep, value, jnp.zeros_like(value))

    def mask_chunk(n, carry):
        high_by, x_by, y_by = n // 4, lax.rem(n // 2, 2), lax.rem(n, 2)
        first = 2 * (4 * apart(high, high_by) + 2 * apart(x, x_by) + apart(y, y_by))
        mask(first)
        mask(first + 1)
        return carry

    def mask_more():
        lax.fori_loop(3, 6, mask_chunk, 0)
        lax.fori_loop(7, 8, mask_chunk, 0)

    for load in loads:
        load.wait()
    lax.fori_loop(0, 3, mask_chunk, 0)
    lax.fori_loop(6, 7, mask_chunk, 0)
    pl.semaphore_wait(barrier, len(everyone))

    def to_far(high_by, x_by, part):
        send_left(0, 0, 2, at_far, column_of(high_by, x_by, 0, part), None)

    fars = [(high_by, x_by, part) for high_by, x_by in ((1, 1), (1, 0), (0, 1), (0, 0)) for part in range(2)]
    for _ in range(WINDOW):
        to_far(*fars.pop(0))
    for part in range(2):
        to_x(0, 0, 1, 0, part)
    own_panel(0, 0)
    mask_more()
    for which in range(4):
        for part in range(2):
            row = group_rows[which]
            live = is_live(row, wrap(mine + part - row + band + band // 2))
            at = 2 * which + part
            keep_lanes[at : at + 1] = jnp.full((1, block), live)
    acc[...] = jnp.zeros_like(acc)

    here = pl.ds(pl.multiple_of(y * slab, slab), slab)
    there = pl.ds(pl.multiple_of(other_y * slab, slab), slab)
    ends = {0: ((1, at_y),), 1: ((1, at_xy), (0, at_x)), 2: ((1, at_far_y), (0, at_far)), 3: ((1, at_far_xy), (0, at_far_x))}

    def finish(part):
        assert all(("cube", source, part) in done for source in range(16))
        for which in (3, 2, 1, 0):
            total = 3.0 * panels[1, which, part].astype(jnp.float32) - 2.0 * masked(1, which, part)
            pure[which, part] = total.astype(pure.dtype)
            for half, device in ends[which]:
                at = 2 * which + half
                rows = there if half else here
                go(remote(pure.at[which, part, rows], final.at[mine + part], end_send.at[at, part],
                          end_recv.at[at, part], device))

    acts = {"x": lambda a, b, w, t: to_x(0, a, b, w, t), "l": take, "n": own_panel,
            "p": lambda s, t: take_panel(0, s, t), "q": lambda s, t: take_panel(1, s, t),
            "m": square_macs, "s": square, "c": cube_macs, "e": finish}
    for name, *numbers in ORDER:
        acts[name](*numbers)

    outs = []

    def put(ref, column):
        copy = pltpu.make_async_copy(ref, out.at[wrap(column - rank + band + band // 2)], load_sem.at[len(outs)])
        copy.start()
        outs.append(copy)

    for part in range(2):
        put(pure.at[0, part, here], mine + part)
        for which in range(4):
            for half, _ in ends[which]:
                x_by, high_by = GROUP[which]
                at = column_of(high_by, x_by, half, part)
                ref = final.at[at]
                remote(ref, ref, end_send.at[0, 0], end_recv.at[2 * which + half, part], at_y).wait_recv()
                put(ref, at)
    for copy in outs:
        copy.wait()
    for copy, wanted in sent:
        only(wanted, copy.wait_send)


def on_grid(blocks, columns):
    _, band, block, _ = blocks.shape
    dma = pltpu.SemaphoreType.DMA
    result = pl.pallas_call(
        grid_kernel,
        out_shape=jax.ShapeDtypeStruct((band, block // 2, block), blocks.dtype),
        in_specs=[pl.BlockSpec(memory_space=pltpu.SMEM), pl.BlockSpec(memory_space=pl.ANY)],
        out_specs=pl.BlockSpec(memory_space=pl.ANY),
        scratch_shapes=[
            pltpu.VMEM((4, band, block, block), blocks.dtype),
            pltpu.VMEM((2, 16, 2, block, block), blocks.dtype),
            pltpu.VMEM((2, 4, 2, block, block), jnp.float32),
            pltpu.VMEM((4, 2, block, block), blocks.dtype),
            pltpu.VMEM((band, block // 2, block), blocks.dtype),
            pltpu.VMEM((8, block), jnp.int32),
            dma((16,)), dma((7, 16)), dma((4, 16)), dma((2, 8, 2, 2)), dma((2, 16, 2)), dma((8, 2)), dma((8, 2)),
        ],
        compiler_params=pltpu.CompilerParams(
            collective_id=0, has_side_effects=True, vmem_limit_bytes=60 * 1024 * 1024
        ),
    )(columns, blocks[0])
    return result[None].astype(jnp.float32)


def from_behind(value, axis, steps):
    count = lax.axis_size(axis)
    pairs = [(source, (source + steps) % count) for source in range(count)]
    return lax.ppermute(value, axis, pairs)


def live_table(columns):
    nrows, band_width = columns.shape
    half_band = band_width // 2
    row_ids = jnp.arange(nrows, dtype=jnp.int32)
    target = (
        row_ids[:, None] + jnp.arange(band_width, dtype=jnp.int32)[None, :] - half_band
    ) % nrows
    return jnp.any(columns[:, None, :] == target[:, :, None], axis=2)


def slot_shift(piece, delta):
    band_width = piece.shape[1]
    if delta >= 0:
        return jnp.concatenate([piece[:, delta:], jnp.zeros_like(piece[:, :delta])], axis=1)
    return jnp.concatenate(
        [jnp.zeros_like(piece[:, :-delta]), piece[:, : band_width + delta]], axis=1
    )


def fetch_band(row_slab, below, above, block_rows, second):
    band_width = row_slab.shape[1]
    pieces = []
    for offset in range(-below, above + 1):
        if offset == 0:
            pieces.append(row_slab)
            continue
        trimmed = (abs(offset) - 1) * block_rows + 1
        if offset > 0:
            outgoing = row_slab[:, : band_width - trimmed]
        else:
            outgoing = row_slab[:, trimmed:]
        if second:
            incoming = from_behind(outgoing, "rows", -offset)
        else:
            incoming = from_behind(outgoing, "rows", -offset)
        filler = jnp.zeros_like(row_slab[:, :trimmed])
        if offset > 0:
            pieces.append(jnp.concatenate([incoming, filler], axis=1))
        else:
            pieces.append(jnp.concatenate([filler, incoming], axis=1))
    return jnp.concatenate(pieces, axis=0)


def merge_groups(totals):
    rounded = lax.optimization_barrier(totals.astype(jnp.bfloat16))
    return jnp.sum(rounded.astype(jnp.float32), axis=0)


def dense_terms(left, window, window_base, groups):
    block_rows, band_width, block_size, inner_width = left.shape
    out_width = window.shape[3]
    half_band = band_width // 2
    group_width = inner_width // groups
    stacked = jnp.stack(
        [
            slot_shift(
                window[window_base + offset : window_base + offset + block_rows], half_band - offset
            )
            for offset in range(band_width)
        ],
        axis=1,
    )
    left_groups = left.reshape(block_rows, band_width, block_size, groups, group_width)
    right_groups = stacked.reshape(
        block_rows, band_width, band_width, groups, group_width, out_width
    )
    totals = jnp.einsum(
        "ramcq,rascqn->crsmn", left_groups, right_groups, preferred_element_type=jnp.float32
    )
    return merge_groups(totals)


def band_terms(left, window, window_base, groups):
    return dense_terms(left, window, window_base, groups)


def per_device(blocks, columns):
    block_rows, band_width, block_size, _ = blocks.shape
    half_band = band_width // 2
    inner_count = lax.axis_size("inner")
    slab_width = block_size // inner_count
    inner_index = lax.axis_index("inner")
    row_owner = lax.axis_index("rows")
    live_own = lax.dynamic_slice_in_dim(live_table(columns), row_owner * block_rows, block_rows, 0)
    live_slots = live_own[:, :, None, None]
    masked = jnp.where(live_slots, blocks, jnp.zeros_like(blocks))
    below = -(-half_band // block_rows)
    above = -(-(half_band - 1) // block_rows)
    window_base = below * block_rows - half_band
    row_slab = lax.dynamic_slice_in_dim(masked, inner_index * slab_width, slab_width, 3)
    window = fetch_band(row_slab, below, above, block_rows, False)
    square = band_terms(masked, window, window_base, inner_count)
    square = jnp.where(live_slots, square, jnp.float32(0.0)).astype(jnp.bfloat16)
    second_window = fetch_band(square, below, above, block_rows, True)
    cubed = band_terms(masked, second_window, window_base, inner_count)
    cubed = jnp.where(live_slots, cubed, jnp.float32(0.0))
    column_slabs = 3.0 * square.astype(jnp.float32) - 2.0 * cubed
    return lax.all_to_all(
        column_slabs.astype(jnp.bfloat16), "inner", split_axis=2, concat_axis=3, tiled=True
    ).astype(column_slabs.dtype)


def solution(mesh):
    in_specs = (P("rows", None, None, None), P())
    out_specs = P("rows", None, "inner", None)

    def step(blocks, columns):
        plain = mesh.shape["rows"] == 16 and mesh.shape["inner"] == 2
        if plain and blocks.shape[:2] == (16, 16) and blocks.shape[2] % 256 == 0:
            chosen = on_grid
        else:
            chosen = per_device
        return jax.shard_map(chosen, mesh=mesh, in_specs=in_specs, out_specs=out_specs, check_vma=False)(
            blocks, columns
        )

    return step
```

```python
import functools

import jax
import jax.numpy as jnp
from jax import lax
from jax.experimental import pallas as pl
from jax.experimental.pallas import tpu as pltpu
from jax.sharding import PartitionSpec as P

MESH = pl.DeviceIdType.MESH

WINDOW = 2
DIAGONAL = ((1, 0, 1),)
EXTRA = ((1, 0),)
GROUP = ((0, 0), (1, 0), (0, 1), (1, 1))
ORDER = (
    ("n", 0, 1), ("x", 1, 1, 0, 0), ("x", 1, 1, 0, 1), ("l", 1, 0, 0, 0, 0), ("n", 1, 0),
("l", 1, 0, 0, 0, 1), ("l", 2, 0, 1, 0, 0), ("x", 0, 0, 0, 0), ("l", 1, 1, 0, 0, 0), ("l", 1, 1, 0, 0, 1),
("l", 2, 0, 1, 0, 1), ("x", 0, 0, 0, 1), ("p", 4, 0), ("l", 3, 0, 0, 0, 0), ("n", 3, 0), ("x", 1, 0, 0, 0),
("l", 2, 0, 0, 0, 0), ("n", 2, 0), ("l", 1, 0, 1, 0, 0), ("p", 5, 0), ("l", 3, 0, 0, 0, 1),
("x", 1, 0, 0, 1), ("n", 1, 1), ("l", 1, 0, 1, 0, 1), ("l", 2, 0, 0, 0, 1), ("n", 3, 1), ("n", 2, 1),
("l", 3, 0, 1, 0, 0), ("x", 1, 0, 1, 0), ("x", 1, 0, 1, 1), ("l", 1, 1, 1, 0, 0), ("p", 7, 0),
("l", 2, 1, 1, 0, 0), ("p", 6, 0), ("l", 3, 0, 1, 0, 1), ("l", 1, 1, 1, 0, 1), ("l", 2, 1, 1, 0, 1),
("s", 0, 0, 0), ("l", 3, 1, 0, 0, 0), ("p", 4, 1), ("p", 5, 1), ("l", 2, 1, 0, 0, 0), ("m", 1, 0, 0, 4),
("m", 2, 0, 0, 4), ("s", 1, 0, 4), ("l", 3, 1, 0, 0, 1), ("p", 7, 1), ("l", 2, 1, 0, 0, 1),
("m", 3, 0, 0, 4), ("p", 6, 1), ("s", 0, 1, 0), ("l", 3, 1, 1, 0, 0), ("m", 1, 1, 0, 4), ("s", 1, 1, 4),
("m", 2, 1, 0, 4), ("l", 3, 1, 1, 0, 1), ("m", 3, 1, 0, 4), ("s", 2, 0, 4), ("q", 4, 0), ("s", 3, 0, 4),
("q", 5, 0), ("c", 0, 0, 1, 4), ("s", 2, 1, 4), ("q", 6, 0), ("s", 3, 1, 4), ("c", 0, 8, 1, 2),
("c", 0, 4, 1, 2), ("c", 0, 12, 1, 2), ("c", 0, 10, 1, 2), ("q", 7, 0), ("c", 0, 6, 8, 2),
("c", 0, 7, 8, 2), ("e", 0), ("q", 4, 1), ("q", 5, 1), ("c", 1, 0, 1, 4), ("c", 1, 8, 1, 2),
("c", 1, 4, 1, 2), ("c", 1, 12, 1, 2), ("q", 6, 1), ("c", 1, 10, 1, 2), ("c", 1, 6, 8, 2), ("q", 7, 1),
("c", 1, 7, 8, 2), ("e", 1),
)


def grid_kernel(columns, raw, out, left, panels, acc, pure, final, keep_lanes, load_sem,
                left_send, left_recv, panel_send, panel_recv, end_send, end_recv):
    band, block = raw.shape[0], raw.shape[1]
    slab = block // 2
    rank, y = lax.axis_index("rows"), lax.axis_index("inner")
    core, x, low, high = rank % 2, (rank // 2) % 2, (rank // 4) % 2, rank // 8
    other_y = 1 - y

    def wrap(value):
        return lax.rem(value, band)

    def flip(bit, by):
        return 1 - bit if by else bit

    def row_at(core_by, x_by, low_by, high_by):
        return 8 * flip(high, high_by) + 4 * flip(low, low_by) + 2 * flip(x, x_by) + flip(core, core_by)

    group_rows = [row_at(0, x_by, 0, high_by) for x_by, high_by in GROUP]
    at_y = {"rows": rank, "inner": other_y}
    at_core = {"rows": row_at(1, 0, 0, 0), "inner": y}
    at_x = {"rows": group_rows[1], "inner": y}
    at_near = {"rows": row_at(0, 0, 1, 0), "inner": y}
    at_far = {"rows": group_rows[2], "inner": y}
    at_xy = {"rows": group_rows[1], "inner": other_y}
    at_far_y = {"rows": group_rows[2], "inner": other_y}
    at_far_x = {"rows": group_rows[3], "inner": y}
    at_far_xy = {"rows": group_rows[3], "inner": other_y}
    everyone = (at_y, at_core, at_x, at_near, at_far, at_xy, at_far_y, at_far_x, at_far_xy)

    barrier = pltpu.get_barrier_semaphore()
    for device in everyone:
        pl.semaphore_signal(barrier, inc=1, device_id=device, device_id_type=MESH)

    loads = []
    for slot in range(band):
        column = wrap(rank + slot + band // 2)
        load = pltpu.make_async_copy(raw.at[slot], left.at[0, column], load_sem.at[slot])
        load.start()
        loads.append(load)

    sent = []

    def remote(source, target, send_sem, recv_sem, device):
        return pltpu.make_async_remote_copy(
            src_ref=source, dst_ref=target, send_sem=send_sem, recv_sem=recv_sem, device_id=device, device_id_type=MESH
        )

    def only(wanted, act):
        if wanted is None:
            act()
        else:
            pl.when(wanted)(act)

    def go(copy, wanted=None):
        only(wanted, copy.start)
        sent.append((copy, wanted))

    def column_of(high_by, x_by, y_by, part):
        return 2 * (4 * flip(high, high_by) + 2 * flip(x, x_by) + flip(y, y_by)) + part

    mine = column_of(0, 0, 0, 0)

    def is_read(row, inner_row, first, count):
        s = wrap(first - row + band + band // 2)
        a = wrap(inner_row - row + band + band // 2)
        return (s + count > band) | ((a - s <= band // 2 - 1 + count) & (s - a <= band // 2 - 1))

    def read_by(which, at, flow, y_by):
        row = group_rows[which]
        if flow == "y":
            return is_read(row, at, column_of(0, 0, 1, 0), 2)
        if y_by:
            return is_read(row, at, column_of(0, 1, 0, 0), 2)
        return is_read(row, at, 2 * (4 * high + 2 * (1 - x)), 4)

    def is_live(row, slot):
        target = wrap(row + slot + band // 2)
        found = columns[row, 0] == target
        for at in range(1, columns.shape[1]):
            found = found | (columns[row, at] == target)
        return jnp.where(found, 1, 0)

    def send_left(flow, source, target, device, at, wanted):
        go(remote(left.at[source, at], left.at[target, at], left_send.at[flow, at], left_recv.at[target, at], device), wanted)

    def to_x(source, high_by, x_by, y_by, part):
        at = column_of(high_by, x_by, y_by, part)
        panel = (high_by, x_by, y_by) == (0, 1, 0)
        wanted = None if panel else read_by(source, at, "x", y_by)
        send_left(1 if source == 0 else 2, source, source + 1, at_x, at, wanted)

    def by_x(which, high_by, x_by, y_by):
        return y_by == 0 or (which == 1 and (high_by, 1 - x_by) in EXTRA)

    done = set()

    def take(which, high_by, x_by, y_by, part):
        key = ("left", which, high_by, x_by, y_by, part)
        if key in done:
            return
        done.add(key)
        at = column_of(high_by, x_by, y_by, part)
        ref = left.at[which, at]
        copy = remote(ref, ref, left_send.at[0, at], left_recv.at[which, at], at_y)
        wanted = None
        if y_by:
            wanted = is_read(group_rows[which], at, mine, 2)
        elif which != 2 and (high_by, x_by) != (0, 0):
            wanted = is_read(group_rows[which], at, 2 * (4 * high + 2 * x), 4)
        only(wanted, copy.wait_recv)
        if y_by:
            return
        if (high_by, x_by) == (0, 0):
            panels[0, which, part] = left[which, mine + part]
        if which == 2 and fars:
            to_far(*fars.pop(0))
        if which == 2:
            to_x(2, high_by, x_by, 0, part)
            if (high_by, x_by, part) in DIAGONAL:
                wanted = is_read(group_rows[2], at, column_of(0, 1, 1, 0), 2)
                send_left(6, 2, 3, at_xy, at, wanted)
        if not (which == 1 and (high_by, 1 - x_by) in EXTRA or which == 3 and (high_by, 1 - x_by, part) in DIAGONAL):
            send_left(2 + which, which, which, at_y, at, read_by(which, at, "y", 0))

    def send_panel(product, source, target, part, device):
        own = product == 0 and source < 4
        ref = left.at[source, mine + part] if own else panels.at[product, source, part]
        go(remote(ref, panels.at[product, target, part], panel_send.at[product, source, target // 8, part],
                  panel_recv.at[product, target, part], device))

    def share(product, which, part):
        send_panel(product, which, 4 + which, part, at_near)
        send_panel(product, which, 8 + which, part, at_core)

    def take_panel(product, source, part):
        key = ("panel", product, source, part)
        if key in done:
            return
        done.add(key)
        ref = panels.at[product, source, part]
        remote(ref, ref, panel_send.at[product, 0, 0, 0], panel_recv.at[product, source, part], at_core).wait_recv()
        if source < 8:
            send_panel(product, source, 8 + source, part, at_core)

    def own_panel(which, part):
        if which:
            take(which, 0, 0, 0, part)
        else:
            panels[0, which, part] = left[which, mine + part]
        share(0, which, part)

    def apart(a, b):
        return a + b - 2 * a * b

    def source_of(row):
        return (8 * apart(row % 2, core) + 4 * apart((row // 4) % 2, low)
                + 2 * apart(row // 8, high) + apart((row // 2) % 2, x))

    def row_of(source):
        return (8 * apart((source // 2) % 2, high) + 4 * apart((source // 4) % 2, low)
                + 2 * apart(source % 2, x) + apart(source // 8, core))

    def mac(product, which, part, terms):
        row = group_rows[which]
        total = None
        for inner_row, source in terms:
            valid = is_read(row, inner_row, mine + part, 1)
            term = jnp.dot(left[which, inner_row], panels[product, source, part], preferred_element_type=jnp.float32)
            term = jnp.where(valid, term, 0.0)
            total = term if total is None else total + term
        acc[product, which, part] += total

    def take_row(which):
        for high_by in range(2 if which else 0):
            for x_by in range(2):
                for y_by in range(2):
                    for part in range(2):
                        take(which, high_by, x_by, y_by, part)

    def square_macs(which, part, first, count):
        for high_by in range(first // 4, (first + count) // 4):
            for x_by in range(2):
                for y_by in range(2):
                    for at in range(2):
                        if which:
                            take(which, high_by, x_by, y_by, at)
        for source in range(1, 4):
            take(source, 0, 0, 0, part)
        for source in range(4, 16):
            take_panel(0, source, part)

        def body(n, carry):
            high_by, x_by, y_by = n // 4, lax.rem(n // 2, 2), lax.rem(n, 2)
            inner_row = 2 * (4 * apart(high, high_by) + 2 * apart(x, x_by) + apart(y, y_by))
            mac(0, which, part, [(inner_row + step, source_of(inner_row + step)) for step in range(2)])
            return carry

        lax.fori_loop(first, first + count, body, 0)
        assert (which, part) not in done
        done.add((which, part, first + count))

    def cube_macs(part, first, stride, count):
        for which in range(4):
            take_row(which)
        for n in range(count):
            source = first + n * stride
            done.add(("cube", source, part))
            if source < 4:
                assert (source, part) in done
            else:
                take_panel(1, source, part)

        def body(n, carry):
            sources = [first + (2 * n + step) * stride for step in range(2)]
            for which in range(4):
                mac(1, which, part, [(row_of(source), source) for source in sources])
            return carry

        lax.fori_loop(0, count // 2, body, 0)

    def masked(product, which, part):
        keep = keep_lanes[2 * which + part : 2 * which + part + 1] > 0
        return jnp.where(keep, acc[product, which, part], 0.0)

    def square(which, part, first):
        assert first == 0 or (which, part, first) in done
        square_macs(which, part, first, 8 - first)
        done.add((which, part))
        panels[1, which, part] = masked(0, which, part).astype(panels.dtype)
        share(1, which, part)

    def mask(column):
        row_slot = wrap(column - rank + band + band // 2)
        keep = jnp.full((1, block), is_live(rank, row_slot)) > 0
        value = left[0, column]
        left[0, column] = jnp.where(keep, value, jnp.zeros_like(value))

    def mask_chunk(n, carry):
        high_by, x_by, y_by = n // 4, lax.rem(n // 2, 2), lax.rem(n, 2)
        first = 2 * (4 * apart(high, high_by) + 2 * apart(x, x_by) + apart(y, y_by))
        mask(first)
        mask(first + 1)
        return carry

    def mask_more():
        lax.fori_loop(3, 6, mask_chunk, 0)
        lax.fori_loop(7, 8, mask_chunk, 0)

    for load in loads:
        load.wait()
    lax.fori_loop(0, 3, mask_chunk, 0)
    lax.fori_loop(6, 7, mask_chunk, 0)
    pl.semaphore_wait(barrier, len(everyone))

    def to_far(high_by, x_by, part):
        send_left(0, 0, 2, at_far, column_of(high_by, x_by, 0, part), None)

    fars = [(high_by, x_by, part) for high_by, x_by in ((1, 1), (1, 0), (0, 1), (0, 0)) for part in range(2)]
    for _ in range(WINDOW):
        to_far(*fars.pop(0))
    for part in range(2):
        to_x(0, 0, 1, 0, part)
    own_panel(0, 0)
    mask_more()
    for which in range(4):
        for part in range(2):
            row = group_rows[which]
            live = is_live(row, wrap(mine + part - row + band + band // 2))
            at = 2 * which + part
            keep_lanes[at : at + 1] = jnp.full((1, block), live)
    acc[...] = jnp.zeros_like(acc)

    here = pl.ds(pl.multiple_of(y * slab, slab), slab)
    there = pl.ds(pl.multiple_of(other_y * slab, slab), slab)
    ends = {0: ((1, at_y),), 1: ((1, at_xy), (0, at_x)), 2: ((1, at_far_y), (0, at_far)), 3: ((1, at_far_xy), (0, at_far_x))}

    def finish(part):
        assert all(("cube", source, part) in done for source in range(16))
        for which in (3, 2, 1, 0):
            total = 3.0 * panels[1, which, part].astype(jnp.float32) - 2.0 * masked(1, which, part)
            pure[which, part] = total.astype(pure.dtype)
            for half, device in ends[which]:
                at = 2 * which + half
                rows = there if half else here
                go(remote(pure.at[which, part, rows], final.at[mine + part], end_send.at[at, part],
                          end_recv.at[at, part], device))

    acts = {"x": lambda a, b, w, t: to_x(0, a, b, w, t), "l": take, "n": own_panel,
            "p": lambda s, t: take_panel(0, s, t), "q": lambda s, t: take_panel(1, s, t),
            "m": square_macs, "s": square, "c": cube_macs, "e": finish}
    for name, *numbers in ORDER:
        acts[name](*numbers)

    outs = []

    def put(ref, column):
        copy = pltpu.make_async_copy(ref, out.at[wrap(column - rank + band + band // 2)], load_sem.at[len(outs)])
        copy.start()
        outs.append(copy)

    for part in range(2):
        put(pure.at[0, part, here], mine + part)
        for which in range(4):
            for half, _ in ends[which]:
                x_by, high_by = GROUP[which]
                at = column_of(high_by, x_by, half, part)
                ref = final.at[at]
                remote(ref, ref, end_send.at[0, 0], end_recv.at[2 * which + half, part], at_y).wait_recv()
                put(ref, at)
    for copy in outs:
        copy.wait()
    for copy, wanted in sent:
        only(wanted, copy.wait_send)


def on_grid(blocks, columns):
    _, band, block, _ = blocks.shape
    dma = pltpu.SemaphoreType.DMA
    result = pl.pallas_call(
        grid_kernel,
        out_shape=jax.ShapeDtypeStruct((band, block // 2, block), blocks.dtype),
        in_specs=[pl.BlockSpec(memory_space=pltpu.SMEM), pl.BlockSpec(memory_space=pl.ANY)],
        out_specs=pl.BlockSpec(memory_space=pl.ANY),
        scratch_shapes=[
            pltpu.VMEM((4, band, block, block), blocks.dtype),
            pltpu.VMEM((2, 16, 2, block, block), blocks.dtype),
            pltpu.VMEM((2, 4, 2, block, block), jnp.float32),
            pltpu.VMEM((4, 2, block, block), blocks.dtype),
            pltpu.VMEM((band, block // 2, block), blocks.dtype),
            pltpu.VMEM((8, block), jnp.int32),
            dma((16,)), dma((7, 16)), dma((4, 16)), dma((2, 8, 2, 2)), dma((2, 16, 2)), dma((8, 2)), dma((8, 2)),
        ],
        compiler_params=pltpu.CompilerParams(
            collective_id=0, has_side_effects=True, vmem_limit_bytes=60 * 1024 * 1024
        ),
    )(columns, blocks[0])
    return result[None].astype(jnp.float32)


def from_behind(value, axis, steps):
    count = lax.axis_size(axis)
    pairs = [(source, (source + steps) % count) for source in range(count)]
    return lax.ppermute(value, axis, pairs)


def live_table(columns):
    nrows, band_width = columns.shape
    half_band = band_width // 2
    row_ids = jnp.arange(nrows, dtype=jnp.int32)
    target = (
        row_ids[:, None] + jnp.arange(band_width, dtype=jnp.int32)[None, :] - half_band
    ) % nrows
    return jnp.any(columns[:, None, :] == target[:, :, None], axis=2)


def slot_shift(piece, delta):
    band_width = piece.shape[1]
    if delta >= 0:
        return jnp.concatenate([piece[:, delta:], jnp.zeros_like(piece[:, :delta])], axis=1)
    return jnp.concatenate(
        [jnp.zeros_like(piece[:, :-delta]), piece[:, : band_width + delta]], axis=1
    )


def fetch_band(row_slab, below, above, block_rows, second):
    band_width = row_slab.shape[1]
    pieces = []
    for offset in range(-below, above + 1):
        if offset == 0:
            pieces.append(row_slab)
            continue
        trimmed = (abs(offset) - 1) * block_rows + 1
        if offset > 0:
            outgoing = row_slab[:, : band_width - trimmed]
        else:
            outgoing = row_slab[:, trimmed:]
        if second:
            incoming = from_behind(outgoing, "rows", -offset)
        else:
            incoming = from_behind(outgoing, "rows", -offset)
        filler = jnp.zeros_like(row_slab[:, :trimmed])
        if offset > 0:
            pieces.append(jnp.concatenate([incoming, filler], axis=1))
        else:
            pieces.append(jnp.concatenate([filler, incoming], axis=1))
    return jnp.concatenate(pieces, axis=0)


def merge_groups(totals):
    rounded = lax.optimization_barrier(totals.astype(jnp.bfloat16))
    return jnp.sum(rounded.astype(jnp.float32), axis=0)


def dense_terms(left, window, window_base, groups):
    block_rows, band_width, block_size, inner_width = left.shape
    out_width = window.shape[3]
    half_band = band_width // 2
    group_width = inner_width // groups
    stacked = jnp.stack(
        [
            slot_shift(
                window[window_base + offset : window_base + offset + block_rows], half_band - offset
            )
            for offset in range(band_width)
        ],
        axis=1,
    )
    left_groups = left.reshape(block_rows, band_width, block_size, groups, group_width)
    right_groups = stacked.reshape(
        block_rows, band_width, band_width, groups, group_width, out_width
    )
    totals = jnp.einsum(
        "ramcq,rascqn->crsmn", left_groups, right_groups, preferred_element_type=jnp.float32
    )
    return merge_groups(totals)


def band_terms(left, window, window_base, groups):
    return dense_terms(left, window, window_base, groups)


def per_device(blocks, columns):
    block_rows, band_width, block_size, _ = blocks.shape
    half_band = band_width // 2
    inner_count = lax.axis_size("inner")
    slab_width = block_size // inner_count
    inner_index = lax.axis_index("inner")
    row_owner = lax.axis_index("rows")
    live_own = lax.dynamic_slice_in_dim(live_table(columns), row_owner * block_rows, block_rows, 0)
    live_slots = live_own[:, :, None, None]
    masked = jnp.where(live_slots, blocks, jnp.zeros_like(blocks))
    below = -(-half_band // block_rows)
    above = -(-(half_band - 1) // block_rows)
    window_base = below * block_rows - half_band
    row_slab = lax.dynamic_slice_in_dim(masked, inner_index * slab_width, slab_width, 3)
    window = fetch_band(row_slab, below, above, block_rows, False)
    square = band_terms(masked, window, window_base, inner_count)
    square = jnp.where(live_slots, square, jnp.float32(0.0)).astype(jnp.bfloat16)
    second_window = fetch_band(square, below, above, block_rows, True)
    cubed = band_terms(masked, second_window, window_base, inner_count)
    cubed = jnp.where(live_slots, cubed, jnp.float32(0.0))
    column_slabs = 3.0 * square.astype(jnp.float32) - 2.0 * cubed
    return lax.all_to_all(
        column_slabs.astype(jnp.bfloat16), "inner", split_axis=2, concat_axis=3, tiled=True
    ).astype(column_slabs.dtype)


def solution(mesh):
    in_specs = (P("rows", None, None, None), P())
    out_specs = P("rows", None, "inner", None)

    def step(blocks, columns):
        plain = mesh.shape["rows"] == 16 and mesh.shape["inner"] == 2
        if plain and blocks.shape[:2] == (16, 16) and blocks.shape[2] % 256 == 0:
            chosen = on_grid
        else:
            chosen = per_device
        return jax.shard_map(chosen, mesh=mesh, in_specs=in_specs, out_specs=out_specs, check_vma=False)(
            blocks, columns
        )

    return step
```
